32 devices in a mesh: row: 4 (over x, core), col: 8 (over z, y).
Axes of the slice: x: 2, y: 2, z: 4, core: 2. Of those that a mesh axis runs over, the one named last changes fastest.
Arguments:
- resistance: float32 [4096, 8192], P('row', 'col'), may hold values from 1 to 100
- source_mask: int32 [4096, 8192], P('row', 'col'), may hold values 0 or 1
- target_mask: int32 [4096, 8192], P('row', 'col'), may hold values 0 or 1
- centers: int32 [512, 2], P(('row', 'col')), may hold values from 0 to 8191, as said below
- live_counts: int32 [32], P(('row', 'col')), may hold values from 1 to 16, 128 in all
Outputs:
- current_map: float32 [4096, 8192], P('row', 'col')
The draws below stay inside these ranges and needn't reach their ends.
Inputs may be any that keep to these rules, and one draw needn't show every extreme that they name: `centers`: the center of slot s lies inside the block of raster cells held by device s // 16 (numbered along row+col, row slowest). Slots 0 to live_counts[d] - 1 of device d are live; some device has all 16 slots live.
All inputs are finite; a program needn't handle non-finite values. No bound on the sum of `source_mask` or of `target_mask` on one device may be relied on, other than what follows from the above.
Results may differ from the reference program's by a relative error of at most 0.0003.
Values sent between devices are 32-bit elements; how exact they have to be, the bound alone decides.
A program may use at most 128 MiB of HBM per device.

```python
import math
import jax
import jax.numpy as jnp
import numpy as np
from jax import lax

TILE_R = 1024
TILE_C = 1024
RAD = 64
ITERS = 24
WCAP = 16
H = 4096
W = 8192
NWIN = 512
DEVICES = 32


def draw_centers(key, part):
    device = jnp.arange(NWIN, dtype=jnp.int32) // WCAP
    col_devices = W // TILE_C
    device_row = device // col_devices
    device_col = device % col_devices
    key_rows = jax.random.fold_in(key, 11)
    key_cols = jax.random.fold_in(key, 23)
    rows_in = jax.random.randint(key_rows, (NWIN,), 0, TILE_R, dtype=jnp.int32)
    cols_in = jax.random.randint(key_cols, (NWIN,), 0, TILE_C, dtype=jnp.int32)
    return jnp.stack([device_row * TILE_R + rows_in, device_col * TILE_C + cols_in], axis=1)


def touch_ends(result, key, smallest, high):
    longest = result.shape.index(max(result.shape))
    spots = []
    for shift in (0, 1):
        where = [jax.random.randint(jax.random.fold_in(key, axis), (), 0, length) for axis, length in enumerate(result.shape)]
        where[longest] = (where[longest] + shift) % result.shape[longest]
        spots.append(tuple(where))
    return result.at[spots[0]].set(smallest).at[spots[1]].set(high)


def steps_of(stream_key, shape, cuts, least, largest):
    gain = 1.0
    for axis_at, parts in cuts:
        heights = jax.random.uniform(jax.random.fold_in(jax.random.fold_in(stream_key, 6), axis_at), (parts,), jnp.float32, least / len(cuts), largest / len(cuts))
        gain = gain * jnp.repeat(jnp.exp(heights), shape[axis_at] // parts).reshape((-1,) + (1,) * (len(shape) - 1 - axis_at))
    return gain


def length_profile(amount, total, limit, lean):
    weights = [(1 << 20) // math.isqrt(standing ** lean) + 1 for standing in range(2, amount + 1)]
    surplus, given = total - limit - (amount - 1), [1] * (amount - 1)
    while surplus > 0:
        free = [i for i in range(amount - 1) if given[i] < limit]
        pool, left = sum([weights[i] for i in free]), surplus
        for i in free:
            extra = min(limit - given[i], max(1, left * weights[i] // pool), surplus)
            given[i] = given[i] + extra
            surplus = surplus - extra
    return np.array([limit] + given)


def uneven_parts(own_key, number_of, total, limit, skew):
    if number_of == 2:
        one = jax.random.randint(own_key, (), max(1, total - limit), min(limit, total - 1) + 1)
        return jnp.stack([one, total - one])
    tallies = jnp.asarray(length_profile(number_of, total, limit, skew), jnp.int32)
    pairs = (number_of - 1) // 2
    donor, receiver = tallies[1:1 + 2 * pairs:2], tallies[2:2 + 2 * pairs:2]
    margin = jnp.minimum(donor - 1, limit - receiver)
    passed = jax.random.randint(jax.random.fold_in(own_key, 1), (pairs,), 0, 1 << 20) % (margin + 1)
    tallies = tallies.at[1:1 + 2 * pairs:2].set(donor - passed).at[2:2 + 2 * pairs:2].set(receiver + passed)
    return tallies[jax.random.permutation(jax.random.fold_in(own_key, 2), number_of)]


def setup_inputs(seed: int = 0) -> dict:
    key_list = jax.random.split(jax.random.key(seed), 6)
    return {
        "resistance": jnp.clip(jnp.exp(math.log(100.0) - 4.6051702 * jax.random.uniform(key_list[0], (H, W), jnp.float32) ** steps_of(key_list[0], (H, W), ((0, 4), (1, 8)), -0.2, 0.2)), 1.0, 100.0),
        "source_mask": touch_ends((jax.random.randint(key_list[1], (H, W), 0, 2) < 1).astype(jnp.int32), jax.random.fold_in(key_list[1], 1), 0, 1),
        "target_mask": touch_ends((jax.random.randint(key_list[2], (H, W), 0, 8) < 1).astype(jnp.int32), jax.random.fold_in(key_list[2], 1), 0, 1),
        "centers": draw_centers(jax.random.fold_in(key_list[5], 71), 0),
        "live_counts": uneven_parts(key_list[4], DEVICES, DEVICES * WCAP // 4, WCAP, 2).astype(jnp.int32),
    }


LEAKAGE = 0.02


def edge_terms(resist):
    inside = (resist > 0.0).astype(jnp.float32)
    safe_res = jnp.where(resist > 0.0, resist, 1.0)
    side_len = resist.shape[-1]
    row_pos = lax.broadcasted_iota(jnp.int32, (side_len, side_len), 0)
    col_pos = lax.broadcasted_iota(jnp.int32, (side_len, side_len), 1)
    not_last_row = (row_pos < side_len - 1).astype(jnp.float32)
    not_last_col = (col_pos < side_len - 1).astype(jnp.float32)
    vertical = not_last_row * inside * jnp.roll(inside, -1, 1) * 2.0 / (safe_res + jnp.roll(safe_res, -1, 1))
    horizontal = not_last_col * inside * jnp.roll(inside, -1, 2) * 2.0 / (safe_res + jnp.roll(safe_res, -1, 2))
    return vertical, horizontal


def window_sum(values):
    return jnp.sum(values, axis=(1, 2), keepdims=True)


def solve_windows(resist, signed):
    vertical, horizontal = edge_terms(resist)
    side_len = resist.shape[-1]
    row_pos = lax.broadcasted_iota(jnp.int32, (side_len, side_len), 0)
    col_pos = lax.broadcasted_iota(jnp.int32, (side_len, side_len), 1)
    center = ((row_pos == RAD) & (col_pos == RAD)).astype(jnp.float32)
    inject = jnp.maximum(signed, 0.0) + center
    ground = jnp.maximum(-signed, 0.0)
    diagonal = vertical + jnp.roll(vertical, 1, 1) + horizontal + jnp.roll(horizontal, 1, 2) + ground + LEAKAGE

    def operate(field):
        beside = vertical * jnp.roll(field, -1, 1) + jnp.roll(vertical * field, 1, 1)
        beside = beside + horizontal * jnp.roll(field, -1, 2) + jnp.roll(horizontal * field, 1, 2)
        return diagonal * field - beside

    voltage = jnp.zeros_like(inject)
    residual = inject
    scaled = residual / diagonal
    direction = scaled
    product_now = window_sum(residual * scaled)
    for repeat in range(ITERS):
        applied = operate(direction)
        step_size = product_now / window_sum(direction * applied)
        voltage = voltage + step_size * direction
        residual = residual - step_size * applied
        scaled = residual / diagonal
        product_next = window_sum(residual * scaled)
        direction = scaled + (product_next / product_now) * direction
        product_now = product_next
    flow_down = vertical * jnp.abs(voltage - jnp.roll(voltage, -1, 1))
    flow_right = horizontal * jnp.abs(voltage - jnp.roll(voltage, -1, 2))
    total_flow = flow_down + jnp.roll(flow_down, 1, 1) + flow_right + jnp.roll(flow_right, 1, 2)
    return 0.5 * (total_flow + inject + ground * jnp.abs(voltage))


def reference(resistance, source_mask, target_mask, centers, live_counts):
    conduct = 1.0 / resistance
    sources = source_mask.astype(jnp.float32)
    targets = target_mask.astype(jnp.float32)
    signed = sources * conduct - targets * (1.0 - sources) * conduct
    side_len = 2 * RAD
    padded_res = jnp.pad(resistance, RAD)
    padded_sign = jnp.pad(signed, RAD)
    accumulated = jnp.zeros((H + 2 * RAD, W + 2 * RAD), jnp.float32)

    def add_window(total_map, slot_index):
        top_row = centers[slot_index, 0].astype(jnp.int32)
        left_col = centers[slot_index, 1].astype(jnp.int32)
        is_live = (slot_index % WCAP < live_counts[slot_index // WCAP]).astype(jnp.float32)
        win_res = lax.dynamic_slice(padded_res, (top_row, left_col), (side_len, side_len))[None]
        win_sign = lax.dynamic_slice(padded_sign, (top_row, left_col), (side_len, side_len))[None]
        current = solve_windows(win_res, win_sign)[0] * is_live
        previous = lax.dynamic_slice(total_map, (top_row, left_col), (side_len, side_len))
        return lax.dynamic_update_slice(total_map, previous + current, (top_row, left_col)), None

    accumulated, unused = lax.scan(add_window, accumulated, jnp.arange(NWIN, dtype=jnp.int32))
    return accumulated[RAD:RAD + H, RAD:RAD + W]
```

```python
import functools

import jax
import jax.numpy as jnp
from jax import lax
from jax.experimental import pallas as pl
from jax.experimental.pallas import tpu as pltpu
from jax.sharding import PartitionSpec as P

RAD = 64
SIDE = 2 * RAD
ITERS = 24
LEAKAGE = 0.02
GROUP = 4
LANES = 128
TALL = SIDE + 8
WIDE = 2 * LANES
SHIFTS = ((-1, 0), (1, 0), (0, -1), (0, 1), (-1, -1), (-1, 1), (1, -1), (1, 1))


def roll(value, shift, axis):
    return pltpu.roll(value, shift % value.shape[axis], axis)


def pack(strip):
    half = strip.shape[-2] // 2
    return jnp.concatenate([strip[..., :half, :], strip[..., half:, :]], axis=-1)


def lane_ids(shape):
    return lax.broadcasted_iota(jnp.int32, shape, 1)


def to_low(packed):
    return packed, roll(packed, RAD, 1)


def to_high(packed):
    return roll(packed, RAD, 1), packed


def pack_low(tile):
    half = tile.shape[0] // 2
    first, second = tile[:half], tile[half:]
    return jnp.where(lane_ids(first.shape) < RAD, first, roll(second, RAD, 1))


def pack_high(tile):
    half = tile.shape[0] // 2
    first, second = tile[:half], tile[half:]
    return jnp.where(lane_ids(first.shape) < RAD, roll(first, RAD, 1), second)


def exchange(pieces):
    rows, cols = lax.axis_size("row"), lax.axis_size("col")
    got = {}
    for (dr, dc) in SHIFTS:
        pairs = [
            (r * cols + c, (r + dr) * cols + c + dc)
            for r in range(rows)
            for c in range(cols)
            if 0 <= r + dr < rows and 0 <= c + dc < cols
        ]
        got[(-dr, -dc)] = lax.ppermute(pieces[(dr, dc)], ("row", "col"), pairs)
    return got


def corner_of(centers, slot, rows, cols):
    return lax.rem(centers[slot, 0], rows) - RAD, lax.rem(centers[slot, 1], cols) - RAD


def is_inner(top, left, rows, cols):
    return (top >= 0) & (top <= rows - SIDE) & (left >= 0) & (left <= cols - SIDE)


def clamped(top, left, rows, cols):
    row = jnp.clip((top + RAD) // 8 * 8 - RAD, 0, rows - TALL)
    col = jnp.clip((left + LANES) // LANES * LANES - LANES, 0, cols - WIDE)
    return pl.multiple_of(row, 8), pl.multiple_of(col, LANES)


def total(values):
    return jnp.sum(jnp.sum(values, axis=0, keepdims=True), axis=1, keepdims=True)


def cut_rows(value, skip):
    return pltpu.roll(value, lax.rem(TALL - skip, TALL), 0)[:SIDE]


def add_window(acc, current, top, left):
    col = pl.multiple_of((left + LANES) // LANES * LANES, LANES)
    shift = left + LANES - col
    wide = jnp.concatenate([current, jnp.zeros_like(current)], axis=1)
    wide = pltpu.roll(wide, shift, 1)
    wide = jnp.concatenate([wide, jnp.zeros((8, WIDE), jnp.float32)], axis=0)
    wide = pltpu.roll(wide, lax.rem(top + RAD, 8), 0)
    rows = pl.ds(pl.multiple_of((top + RAD) // 8 * 8, 8), TALL)
    acc[rows, pl.ds(col, WIDE)] = acc[rows, pl.ds(col, WIDE)] + wide


def solve_kernel(border, rows, cols, *refs):
    centers, live, res_in, src_in, tgt_in = refs[:5]
    if border:
        halos = dict(zip(SHIFTS, refs[5:13]))
        cur, outs, rest = refs[13], dict(zip(SHIFTS, refs[14:22])), refs[22:]
    else:
        cur, rest = refs[5], refs[6:]
    res_buf, src_buf, tgt_buf, sems, order = rest[:5]
    r_s, p_s, s_s, x_s, w_s, vd_s, vu_s, hr_s, hl_s, isd_s, inj_s, gnd_s, v_s, h_s = rest[5:19]
    slots = centers.shape[0]

    def copies(slot):
        top, left = corner_of(centers, slot, rows, cols)
        row, col = clamped(top, left, rows, cols)
        return [
            pltpu.make_async_copy(
                src.at[pl.ds(row, TALL), pl.ds(col, WIDE)],
                dst.at[slot, pl.ds(RAD, TALL), :],
                sems.at[k, slot],
            )
            for k, (src, dst) in enumerate(((res_in, res_buf), (src_in, src_buf), (tgt_in, tgt_buf)))
        ]

    def classify(slot, count):
        top, left = corner_of(centers, slot, rows, cols)
        inner = is_inner(top, left, rows, cols)
        mine = jnp.logical_not(inner) if border else inner

        @pl.when(mine)
        def _():
            order[count] = slot
            for copy in copies(slot):
                copy.start()

        return count + mine.astype(jnp.int32)

    count = lax.fori_loop(0, live[0], classify, jnp.int32(0))

    if border:
        ext, acc = rest[19], rest[20]
        acc[...] = jnp.zeros_like(acc)
        spans = {
            -1: (slice(0, RAD), slice(0, LANES)),
            0: (slice(RAD, RAD + rows), slice(LANES, LANES + cols)),
            1: (slice(RAD + rows, SIDE + rows), slice(LANES + cols, WIDE + cols)),
        }
        for which in range(2):
            for dr in (-1, 1):
                ext[which, spans[dr][0], spans[0][1]] = halos[(dr, 0)][which]
            for dr in (-1, 0, 1):
                start, stop = spans[dr][0].start, spans[dr][0].stop
                middle = (start + stop) // 2
                for dc in (-1, 1):
                    split = to_high if dc < 0 else to_low
                    first, second = split(halos[(dr, dc)][which])
                    ext[which, start:middle, spans[dc][1]] = first
                    ext[which, middle:stop, spans[dc][1]] = second

    row_id = lax.broadcasted_iota(jnp.int32, (SIDE, SIDE), 0)
    col_id = lax.broadcasted_iota(jnp.int32, (SIDE, SIDE), 1)

    def operate(b):
        here = r_s[b, 8:8 + SIDE, :]
        down = r_s[b, 9:9 + SIDE, :]
        up = r_s[b, 7:7 + SIDE, :]
        beside = vd_s[b] * down + vu_s[b] * up
        beside = beside + hr_s[b] * roll(here, -1, 1) + hl_s[b] * roll(here, 1, 1)
        applied = here - beside
        w_s[b] = applied
        return total(here * here), total(here * applied)

    def prepare(b, slot):
        top, left = corner_of(centers, slot, rows, cols)
        row, col = clamped(top, left, rows, cols)
        take = pl.ds(pl.multiple_of((RAD + top - row) // 8 * 8, 8), TALL)
        skip = lax.rem(RAD + top - row, 8)
        res = res_buf[slot, take, :]
        source = src_buf[slot, take, :].astype(jnp.float32)
        target = tgt_buf[slot, take, :].astype(jnp.float32)
        mark = source - target * (1.0 - source)
        turn = lax.rem(WIDE + col - left, WIDE)
        res = cut_rows(pltpu.roll(res, turn, 1)[:, :SIDE], skip)
        mark = cut_rows(pltpu.roll(mark, turn, 1)[:, :SIDE], skip)
        if border:
            at_row, at_col = row_id + top, col_id + left
            own = (at_row >= 0) & (at_row < rows) & (at_col >= 0) & (at_col < cols)
            base = pl.multiple_of((left + LANES) // LANES * LANES, LANES)
            back = lax.rem(WIDE + base - left - LANES, WIDE)
            span = pl.ds(pl.multiple_of((top + RAD) // 8 * 8, 8), TALL)
            outer = [
                cut_rows(pltpu.roll(ext[k, span, pl.ds(base, WIDE)], back, 1)[:, :SIDE], lax.rem(top + RAD, 8))
                for k in range(2)
            ]
            signed = jnp.where(own, mark / jnp.where(own, res, 1.0), outer[1])
            res = jnp.where(own, res, outer[0])
        else:
            signed = mark / res
        res_down, res_right = roll(res, -1, 0), roll(res, -1, 1)
        has_down = (res > 0.0) & (res_down > 0.0) & (row_id < SIDE - 1)
        has_right = (res > 0.0) & (res_right > 0.0) & (col_id < SIDE - 1)
        vertical = jnp.where(has_down, 2.0 / jnp.where(has_down, res + res_down, 1.0), 0.0)
        horizontal = jnp.where(has_right, 2.0 / jnp.where(has_right, res + res_right, 1.0), 0.0)
        center = ((row_id == RAD) & (col_id == RAD)).astype(jnp.float32)
        inject = jnp.maximum(signed, 0.0) + center
        ground = jnp.maximum(-signed, 0.0)
        diagonal = vertical + roll(vertical, 1, 0) + horizontal + roll(horizontal, 1, 1) + ground + LEAKAGE
        isd = 1.0 / jnp.sqrt(diagonal)
        scaled_v = vertical * isd * roll(isd, -1, 0)
        scaled_h = horizontal * isd * roll(isd, -1, 1)
        v_s[b], h_s[b] = vertical, horizontal
        vd_s[b], vu_s[b] = scaled_v, roll(scaled_v, 1, 0)
        hr_s[b], hl_s[b] = scaled_h, roll(scaled_h, 1, 1)
        inj_s[b], gnd_s[b], isd_s[b] = inject, ground, isd
        r_s[b, 0:8, :] = jnp.zeros((8, SIDE), jnp.float32)
        r_s[b, 8 + SIDE:16 + SIDE, :] = jnp.zeros((8, SIDE), jnp.float32)
        r_s[b, 8:8 + SIDE, :] = inject * isd
        zero = jnp.zeros((SIDE, SIDE), jnp.float32)
        p_s[b], s_s[b], x_s[b] = zero, zero, zero

    def step(_, carry):
        after = []
        for b in range(GROUP):
            gamma, alpha, beta = carry[b]
            here = r_s[b, 8:8 + SIDE, :]
            direction = here + beta * p_s[b]
            applied = w_s[b] + beta * s_s[b]
            p_s[b] = direction
            s_s[b] = applied
            x_s[b] = x_s[b] + alpha * direction
            r_s[b, 8:8 + SIDE, :] = here - alpha * applied
        for b in range(GROUP):
            gamma, alpha, beta = carry[b]
            gamma_next, delta = operate(b)
            beta_next = gamma_next / gamma
            alpha_next = gamma_next / (delta - beta_next * gamma_next / alpha)
            after.append((gamma_next, alpha_next, beta_next))
        return tuple(after)

    def finish(b, slot):
        isd, vertical, horizontal = isd_s[b], v_s[b], h_s[b]
        voltage = x_s[b] * isd
        flow_down = vertical * jnp.abs(voltage - roll(voltage, -1, 0))
        flow_right = horizontal * jnp.abs(voltage - roll(voltage, -1, 1))
        flow = flow_down + roll(flow_down, 1, 0) + flow_right + roll(flow_right, 1, 1)
        current = 0.5 * (flow + inj_s[b] + gnd_s[b] * jnp.abs(voltage))
        cur[slot] = current
        return current

    def solve_group(group, _):
        def ready(b, _):
            at = group * GROUP + b
            slot = order[jnp.minimum(at, count - 1)]

            @pl.when(at < count)
            def _():
                for copy in copies(slot):
                    copy.wait()

            prepare(b, slot)
            return 0

        lax.fori_loop(0, GROUP, ready, 0)
        carry = []
        for b in range(GROUP):
            gamma, delta = operate(b)
            carry.append((gamma, gamma / delta, jnp.zeros_like(gamma)))
        lax.fori_loop(0, ITERS, step, tuple(carry))

        def done(b, _):
            at = group * GROUP + b

            @pl.when(at < count)
            def _():
                slot = order[at]
                current = finish(b, slot)
                if border:
                    top, left = corner_of(centers, slot, rows, cols)
                    add_window(acc, current, top, left)

            return 0

        lax.fori_loop(0, GROUP, done, 0)
        return 0

    lax.fori_loop(0, (count + GROUP - 1) // GROUP, solve_group, 0)

    if border:
        for dr in (-1, 1):
            outs[(dr, 0)][...] = acc[spans[dr][0], spans[0][1]]
        for dr in (-1, 0, 1):
            for dc in (-1, 1):
                tile = acc[spans[dr][0], spans[dc][1]]
                outs[(dr, dc)][...] = pack_high(tile) if dc < 0 else pack_low(tile)


def assemble_kernel(rows, cols, centers, live, inner_cur, outer_cur, out, acc, sem):
    acc[...] = jnp.zeros_like(acc)

    def place(slot, _):
        top, left = corner_of(centers, slot, rows, cols)
        inner = is_inner(top, left, rows, cols)

        @pl.when(inner)
        def _():
            add_window(acc, inner_cur[slot], top, left)

        @pl.when(jnp.logical_not(inner))
        def _():
            add_window(acc, outer_cur[slot], top, left)

        return 0

    lax.fori_loop(0, live[0], place, 0)
    copy = pltpu.make_async_copy(acc.at[pl.ds(RAD, rows), pl.ds(LANES, cols)], out, sem)
    copy.start()
    copy.wait()


def fold_kernel(rows, cols, *refs):
    halos = dict(zip(SHIFTS, refs[1:9]))
    out, upper, lower, left, right, sems = refs[9:]
    last = cols - LANES
    inner_rows = rows - SIDE
    places = (
        (upper, pl.ds(0, RAD), pl.ds(0, cols)),
        (lower, pl.ds(rows - RAD, RAD), pl.ds(0, cols)),
        (left, pl.ds(RAD, inner_rows), pl.ds(0, LANES)),
        (right, pl.ds(RAD, inner_rows), pl.ds(last, LANES)),
    )
    fetch = [pltpu.make_async_copy(out.at[r, c], buf, sems.at[0, k]) for k, (buf, r, c) in enumerate(places)]
    store = [pltpu.make_async_copy(buf, out.at[r, c], sems.at[1, k]) for k, (buf, r, c) in enumerate(places)]
    for copy in fetch:
        copy.start()

    def spread(dr, dc):
        first, second = (to_low if dc < 0 else to_high)(halos[(dr, dc)][...])
        low = lane_ids(first.shape) < RAD
        keep = low if dc < 0 else jnp.logical_not(low)
        return jnp.where(keep, first, 0.0), jnp.where(keep, second, 0.0)

    for copy in fetch:
        copy.wait()
    half = rows // 2
    for dc, buf, at in ((-1, left, 0), (1, right, last)):
        first, second = spread(0, dc)
        buf[0:half - RAD] = buf[0:half - RAD] + first[RAD:]
        buf[half - RAD:inner_rows] = buf[half - RAD:inner_rows] + second[:half - RAD]
        upper[:, at:at + LANES] = upper[:, at:at + LANES] + first[:RAD]
        lower[:, at:at + LANES] = lower[:, at:at + LANES] + second[half - RAD:]
        for dr, strip in ((-1, upper), (1, lower)):
            one, two = spread(dr, dc)
            strip[:RAD // 2, at:at + LANES] = strip[:RAD // 2, at:at + LANES] + one
            strip[RAD // 2:, at:at + LANES] = strip[RAD // 2:, at:at + LANES] + two
    upper[...] = upper[...] + halos[(-1, 0)][...]
    lower[...] = lower[...] + halos[(1, 0)][...]
    for copy in store:
        copy.start()
    for copy in store:
        copy.wait()


def local(resistance, source_mask, target_mask, centers, live_counts):
    rows, cols = resistance.shape
    slots = centers.shape[0]
    f32, i32 = jnp.float32, jnp.int32
    smem = pl.BlockSpec(memory_space=pltpu.SMEM)
    vmem = pl.BlockSpec(memory_space=pltpu.VMEM)
    hbm = pl.BlockSpec(memory_space=pl.ANY)

    def edge(at_rows, at_cols):
        res = resistance[at_rows, at_cols]
        sources = source_mask[at_rows, at_cols].astype(f32)
        targets = target_mask[at_rows, at_cols].astype(f32)
        conduct = 1.0 / res
        return jnp.stack([res, sources * conduct - targets * (1.0 - sources) * conduct])

    near = {-1: slice(0, RAD), 0: slice(None), 1: None}
    row_cut = {**near, 1: slice(rows - RAD, rows)}
    col_cut = {**near, 1: slice(cols - RAD, cols)}
    pieces = {}
    for (dr, dc) in SHIFTS:
        piece = edge(row_cut[dr], col_cut[dc])
        pieces[(dr, dc)] = piece if dc == 0 else pack(piece)
    halos = exchange(pieces)

    def solver(border, *extra):
        window = pltpu.VMEM((GROUP, SIDE, SIDE), f32)
        scratch = [
            pltpu.VMEM((slots, TALL + SIDE, WIDE), f32),
            pltpu.VMEM((slots, TALL + SIDE, WIDE), i32),
            pltpu.VMEM((slots, TALL + SIDE, WIDE), i32),
            pltpu.SemaphoreType.DMA((3, slots)),
            pltpu.SMEM((slots,), i32),
            pltpu.VMEM((GROUP, SIDE + 16, SIDE), f32),
        ] + [window] * 13
        out_shape = [jax.ShapeDtypeStruct((slots, SIDE, SIDE), f32)]
        if border:
            scratch += [pltpu.VMEM((2, rows + SIDE, cols + WIDE), f32), pltpu.VMEM((rows + SIDE, cols + WIDE), f32)]
            out_shape += [jax.ShapeDtypeStruct(halos[at].shape[1:], f32) for at in SHIFTS]
        return pl.pallas_call(
            functools.partial(solve_kernel, border, rows, cols),
            out_shape=out_shape,
            in_specs=[smem, smem, hbm, hbm, hbm] + [vmem] * len(extra),
            out_specs=[vmem] * len(out_shape),
            scratch_shapes=scratch,
            compiler_params=pltpu.CompilerParams(vmem_limit_bytes=50 << 20),
            cost_estimate=pl.CostEstimate(
                flops=(30_000_000 if not border else 10_000_000) * 10, bytes_accessed=30_000_000, transcendentals=0
            ),
            name="border" if border else "inner",
        )(centers, live_counts, resistance, source_mask, target_mask, *extra)

    (inner_cur,) = solver(False)
    outer_cur, *strips = solver(True, *[halos[at] for at in SHIFTS])
    back = exchange(dict(zip(SHIFTS, strips)))

    out_shape = jax.ShapeDtypeStruct((rows, cols), f32)
    merged = pl.pallas_call(
        functools.partial(assemble_kernel, rows, cols),
        out_shape=out_shape,
        in_specs=[smem, smem, vmem, vmem],
        out_specs=hbm,
        scratch_shapes=[pltpu.VMEM((rows + SIDE, cols + WIDE), f32), pltpu.SemaphoreType.DMA],
        compiler_params=pltpu.CompilerParams(vmem_limit_bytes=20 << 20),
        cost_estimate=pl.CostEstimate(flops=4_000_000, bytes_accessed=16_000_000, transcendentals=0),
        name="assemble",
    )(centers, live_counts, inner_cur, outer_cur)

    return pl.pallas_call(
        functools.partial(fold_kernel, rows, cols),
        out_shape=out_shape,
        in_specs=[hbm] + [vmem] * 8,
        out_specs=hbm,
        scratch_shapes=[
            pltpu.VMEM((RAD, cols), f32),
            pltpu.VMEM((RAD, cols), f32),
            pltpu.VMEM((rows - SIDE, LANES), f32),
            pltpu.VMEM((rows - SIDE, LANES), f32),
            pltpu.SemaphoreType.DMA((2, 4)),
        ],
        input_output_aliases={0: 0},
        compiler_params=pltpu.CompilerParams(vmem_limit_bytes=16 << 20),
        name="fold",
    )(merged, *[back[at] for at in SHIFTS])


def solution(mesh):
    return jax.shard_map(
        local,
        mesh=mesh,
        in_specs=(
            P("row", "col"),
            P("row", "col"),
            P("row", "col"),
            P(("row", "col"), None),
            P(("row", "col")),
        ),
        out_specs=P("row", "col"),
        check_vma=False,
    )
```

```python
import functools

import jax
import jax.numpy as jnp
from jax import lax
from jax.experimental import pallas as pl
from jax.experimental.pallas import tpu as pltpu
from jax.sharding import PartitionSpec as P

RAD = 64
SIDE = 2 * RAD
ITERS = 24
LEAKAGE = 0.02
GROUP = 4
LANES = 128
TALL = SIDE + 8
WIDE = 2 * LANES
SHIFTS = ((0, -1), (0, 1), (-1, 0), (1, 0), (-1, -1), (-1, 1), (1, -1), (1, 1))


def roll(value, shift, axis):
    return pltpu.roll(value, shift % value.shape[axis], axis)


def lane_ids(shape):
    return lax.broadcasted_iota(jnp.int32, shape, 1)


def to_low(packed):
    return packed, roll(packed, RAD, 1)


def to_high(packed):
    return roll(packed, RAD, 1), packed


def pack_low(tile):
    half = tile.shape[0] // 2
    first, second = tile[:half], tile[half:]
    return jnp.where(lane_ids(first.shape) < RAD, first, roll(second, RAD, 1))


def pack_high(tile):
    half = tile.shape[0] // 2
    first, second = tile[:half], tile[half:]
    return jnp.where(lane_ids(first.shape) < RAD, roll(first, RAD, 1), second)


def neighbours():
    row, col = lax.axis_index("row"), lax.axis_index("col")
    rows, cols = lax.axis_size("row"), lax.axis_size("col")
    found = {}
    for (dr, dc) in SHIFTS:
        r, c = row + dr, col + dc
        found[(dr, dc)] = ((r >= 0) & (r < rows) & (c >= 0) & (c < cols), (r, c))
    return found


def greet(found):
    barrier = pltpu.get_barrier_semaphore()
    for at in SHIFTS:
        exists, device = found[at]

        @pl.when(exists)
        def _():
            pl.semaphore_signal(barrier, inc=1, device_id=device, device_id_type=pl.DeviceIdType.MESH)


def all_greeted(found):
    count = sum(found[at][0].astype(jnp.int32) for at in SHIFTS)
    pl.semaphore_wait(pltpu.get_barrier_semaphore(), count)


def transfers(found, pieces, halos, send_sems, recv_sems):
    made = []
    for k, at in enumerate(SHIFTS):
        exists, device = found[at]
        back = (-at[0], -at[1])
        made.append((exists, pltpu.make_async_remote_copy(
            src_ref=pieces[at],
            dst_ref=halos[back],
            send_sem=send_sems.at[k],
            recv_sem=recv_sems.at[SHIFTS.index(back)],
            device_id=device,
            device_id_type=pl.DeviceIdType.MESH,
        )))
    return made


def landings(found, pieces, halos, send_sems, recv_sems):
    made = []
    for k, at in enumerate(SHIFTS):
        exists, device = found[at]
        made.append((exists, pltpu.make_async_remote_copy(
            src_ref=pieces[at],
            dst_ref=halos[at],
            send_sem=send_sems.at[k],
            recv_sem=recv_sems.at[k],
            device_id=device,
            device_id_type=pl.DeviceIdType.MESH,
        )))
    return made


def start_all(copies):
    for exists, copy in copies:
        pl.when(exists)(copy.start)


def finish_all(copies, arrivals):
    for exists, copy in copies:
        pl.when(exists)(copy.wait_send)
    for exists, copy in arrivals:
        pl.when(exists)(copy.wait_recv)


def corner_of(centers, slot, rows, cols):
    return lax.rem(centers[slot, 0], rows) - RAD, lax.rem(centers[slot, 1], cols) - RAD


def is_inner(top, left, rows, cols):
    return (top >= 0) & (top <= rows - SIDE) & (left >= 0) & (left <= cols - SIDE)


def clamped(top, left, rows, cols):
    row = jnp.clip((top + RAD) // 8 * 8 - RAD, 0, rows - TALL)
    col = jnp.clip((left + LANES) // LANES * LANES - LANES, 0, cols - WIDE)
    return pl.multiple_of(row, 8), pl.multiple_of(col, LANES)


def total(values):
    return jnp.sum(jnp.sum(values, axis=0, keepdims=True), axis=1, keepdims=True)


def cut_rows(value, skip):
    return pltpu.roll(value, lax.rem(TALL - skip, TALL), 0)[:SIDE]


def add_window(acc, current, top, left):
    col = pl.multiple_of((left + LANES) // LANES * LANES, LANES)
    shift = left + LANES - col
    wide = jnp.concatenate([current, jnp.zeros_like(current)], axis=1)
    wide = pltpu.roll(wide, shift, 1)
    wide = jnp.concatenate([wide, jnp.zeros((8, WIDE), jnp.float32)], axis=0)
    wide = pltpu.roll(wide, lax.rem(top + RAD, 8), 0)
    rows = pl.ds(pl.multiple_of((top + RAD) // 8 * 8, 8), TALL)
    acc[rows, pl.ds(col, WIDE)] = acc[rows, pl.ds(col, WIDE)] + wide


def solver_parts(state):
    r_s, p_s, s_s, x_s, w_s, vd_s, vu_s, hr_s, hl_s, isd_s, inj_s, gnd_s, v_s, h_s = state
    row_id = lax.broadcasted_iota(jnp.int32, (SIDE, SIDE), 0)
    col_id = lax.broadcasted_iota(jnp.int32, (SIDE, SIDE), 1)

    def operate(b):
        here = r_s[b, 8:8 + SIDE, :]
        down = r_s[b, 9:9 + SIDE, :]
        up = r_s[b, 7:7 + SIDE, :]
        beside = vd_s[b] * down + vu_s[b] * up
        beside = beside + hr_s[b] * roll(here, -1, 1) + hl_s[b] * roll(here, 1, 1)
        applied = here - beside
        w_s[b] = applied
        return total(here * here), total(here * applied)

    def prepare(b, res, signed):
        res_down, res_right = roll(res, -1, 0), roll(res, -1, 1)
        has_down = (res > 0.0) & (res_down > 0.0) & (row_id < SIDE - 1)
        has_right = (res > 0.0) & (res_right > 0.0) & (col_id < SIDE - 1)
        vertical = jnp.where(has_down, 2.0 / jnp.where(has_down, res + res_down, 1.0), 0.0)
        horizontal = jnp.where(has_right, 2.0 / jnp.where(has_right, res + res_right, 1.0), 0.0)
        center = ((row_id == RAD) & (col_id == RAD)).astype(jnp.float32)
        inject = jnp.maximum(signed, 0.0) + center
        ground = jnp.maximum(-signed, 0.0)
        diagonal = vertical + roll(vertical, 1, 0) + horizontal + roll(horizontal, 1, 1) + ground + LEAKAGE
        isd = 1.0 / jnp.sqrt(diagonal)
        scaled_v = vertical * isd * roll(isd, -1, 0)
        scaled_h = horizontal * isd * roll(isd, -1, 1)
        v_s[b], h_s[b] = vertical, horizontal
        vd_s[b], vu_s[b] = scaled_v, roll(scaled_v, 1, 0)
        hr_s[b], hl_s[b] = scaled_h, roll(scaled_h, 1, 1)
        inj_s[b], gnd_s[b], isd_s[b] = inject, ground, isd
        r_s[b, 0:8, :] = jnp.zeros((8, SIDE), jnp.float32)
        r_s[b, 8 + SIDE:16 + SIDE, :] = jnp.zeros((8, SIDE), jnp.float32)
        r_s[b, 8:8 + SIDE, :] = inject * isd
        zero = jnp.zeros((SIDE, SIDE), jnp.float32)
        p_s[b], s_s[b], x_s[b] = zero, zero, zero

    def step(_, carry):
        after = []
        for b in range(GROUP):
            gamma, alpha, beta = carry[b]
            here = r_s[b, 8:8 + SIDE, :]
            direction = here + beta * p_s[b]
            applied = w_s[b] + beta * s_s[b]
            p_s[b] = direction
            s_s[b] = applied
            x_s[b] = x_s[b] + alpha * direction
            r_s[b, 8:8 + SIDE, :] = here - alpha * applied
        for b in range(GROUP):
            gamma, alpha, beta = carry[b]
            gamma_next, delta = operate(b)
            beta_next = gamma_next / gamma
            alpha_next = gamma_next / (delta - beta_next * gamma_next / alpha)
            after.append((gamma_next, alpha_next, beta_next))
        return tuple(after)

    def finish(b):
        isd, vertical, horizontal = isd_s[b], v_s[b], h_s[b]
        voltage = x_s[b] * isd
        flow_down = vertical * jnp.abs(voltage - roll(voltage, -1, 0))
        flow_right = horizontal * jnp.abs(voltage - roll(voltage, -1, 1))
        flow = flow_down + roll(flow_down, 1, 0) + flow_right + roll(flow_right, 1, 1)
        return 0.5 * (flow + inj_s[b] + gnd_s[b] * jnp.abs(voltage))

    def iterate():
        carry = []
        for b in range(GROUP):
            gamma, delta = operate(b)
            carry.append((gamma, gamma / delta, jnp.zeros_like(gamma)))
        lax.fori_loop(0, ITERS, step, tuple(carry))

    return prepare, iterate, finish


def spans_of(rows, cols):
    return {
        -1: (slice(0, RAD), slice(0, LANES)),
        0: (slice(RAD, RAD + rows), slice(LANES, LANES + cols)),
        1: (slice(RAD + rows, SIDE + rows), slice(LANES + cols, WIDE + cols)),
    }


def turn_own(res, source, target, skip, turn):
    source, target = source.astype(jnp.float32), target.astype(jnp.float32)
    mark = source - target * (1.0 - source)
    turn = lax.rem(WIDE + turn, WIDE)
    res = cut_rows(pltpu.roll(res, turn, 1)[:, :SIDE], skip)
    mark = cut_rows(pltpu.roll(mark, turn, 1)[:, :SIDE], skip)
    return res, mark


def cut_kernel(rows, cols, centers, live, *refs):
    raw, out, bufs, sems = refs[:3], refs[3], refs[4:7], refs[7]

    def place(slot):
        top, left = corner_of(centers, slot, rows, cols)
        return top, left, *clamped(top, left, rows, cols)

    def copies(slot):
        _, _, row, col = place(slot)
        return [
            pltpu.make_async_copy(src.at[pl.ds(row, TALL), pl.ds(col, WIDE)], dst.at[slot], sems.at[k, slot])
            for k, (src, dst) in enumerate(zip(raw, bufs))
        ]

    def begin(slot, _):
        for copy in copies(slot):
            copy.start()
        return 0

    def cut(slot, _):
        for copy in copies(slot):
            copy.wait()
        top, left, row, col = place(slot)
        res, mark = turn_own(*(buf[slot] for buf in bufs), top - row, col - left)
        out[0, slot] = res
        out[1, slot] = mark / res
        return 0

    lax.fori_loop(0, live[0], begin, 0)
    lax.fori_loop(0, live[0], cut, 0)


def inner_kernel(rows, cols, windows, *refs):
    raw = refs[:3]
    cur, outs = refs[3], dict(zip(SHIFTS, refs[4:12]))
    pieces, halos = dict(zip(SHIFTS, refs[12:20])), dict(zip(SHIFTS, refs[20:28]))
    frames = [refs[28 + 3 * k:31 + 3 * k] for k in range(4)]
    sems, send_sems, recv_sems = refs[40:43]
    prepare, iterate, finish = solver_parts(refs[43:])
    slots = windows.shape[1]
    found = neighbours()

    everything = pl.ds(0, rows)
    places = (
        (everything, pl.ds(0, LANES)),
        (everything, pl.ds(cols - LANES, LANES)),
        (pl.ds(0, RAD), pl.ds(0, cols)),
        (pl.ds(rows - RAD, RAD), pl.ds(0, cols)),
    )
    frame_copies = [
        [pltpu.make_async_copy(raw[k].at[places[f]], frames[f][k], sems.at[f, k]) for k in range(3)]
        for f in range(4)
    ]
    for copy in sum(frame_copies, []):
        copy.start()
    for at in SHIFTS:
        halos[at][...] = jnp.zeros_like(halos[at])
    greet(found)

    def strengths(frame, cut=slice(None)):
        res, source, target = (ref[cut] for ref in frame)
        source, target = source.astype(jnp.float32), target.astype(jnp.float32)
        conduct = 1.0 / res
        return res, source * conduct - target * (1.0 - source) * conduct

    for f, at in enumerate(((0, -1), (0, 1), (-1, 0), (1, 0))):
        for copy in frame_copies[f]:
            copy.wait()
        for k, value in enumerate(strengths(frames[f])):
            if at[1] == 0:
                pieces[at][k] = value
            else:
                squeeze = pack_low if at[1] < 0 else pack_high
                pieces[at][k] = squeeze(value)
                pieces[(-1, at[1])][k] = squeeze(value[:RAD])
                pieces[(1, at[1])][k] = squeeze(value[rows - RAD:])
    all_greeted(found)
    copies = transfers(found, pieces, halos, send_sems, recv_sems)
    start_all(copies)

    def solve_group(group, _):
        def ready(b, _):
            slot = group * GROUP + b
            prepare(b, windows[0, slot], windows[1, slot])
            return 0

        lax.fori_loop(0, GROUP, ready, 0)
        iterate()

        def done(b, _):
            cur[group * GROUP + b] = finish(b)
            return 0

        lax.fori_loop(0, GROUP, done, 0)
        return 0

    lax.fori_loop(0, slots // GROUP, solve_group, 0)
    finish_all(copies, landings(found, pieces, halos, send_sems, recv_sems))
    for at in SHIFTS:
        outs[at][...] = halos[at][...]


def return_kernel(*refs):
    pieces, outs, halos = (dict(zip(SHIFTS, refs[8 * k:8 * k + 8])) for k in range(3))
    send_sems, recv_sems = refs[24:]
    found = neighbours()
    for at in SHIFTS:
        halos[at][...] = jnp.zeros_like(halos[at])
    greet(found)
    all_greeted(found)
    copies = transfers(found, pieces, halos, send_sems, recv_sems)
    start_all(copies)
    finish_all(copies, landings(found, pieces, halos, send_sems, recv_sems))
    for at in SHIFTS:
        outs[at][...] = halos[at][...]


def border_kernel(rows, cols, centers, live, inner_cur, *refs):
    raw, halos = refs[:3], dict(zip(SHIFTS, refs[3:11]))
    out, outs = refs[11], dict(zip(SHIFTS, refs[12:20]))
    bufs, sems, order, ext, acc, out_sem = refs[20:23], *refs[23:28]
    prepare, iterate, finish = solver_parts(refs[28:])

    def copies(slot):
        top, left = corner_of(centers, slot, rows, cols)
        row, col = clamped(top, left, rows, cols)
        return [
            pltpu.make_async_copy(
                src.at[pl.ds(row, TALL), pl.ds(col, WIDE)],
                dst.at[slot, pl.ds(RAD, TALL), :],
                sems.at[k, slot],
            )
            for k, (src, dst) in enumerate(zip(raw, bufs))
        ]

    def classify(slot, count):
        top, left = corner_of(centers, slot, rows, cols)
        outer = jnp.logical_not(is_inner(top, left, rows, cols))

        @pl.when(outer)
        def _():
            order[count] = slot
            for copy in copies(slot):
                copy.start()

        return count + outer.astype(jnp.int32)

    count = lax.fori_loop(0, live[0], classify, jnp.int32(0))
    acc[...] = jnp.zeros_like(acc)
    spans = spans_of(rows, cols)
    for which in range(2):
        for dr in (-1, 1):
            ext[which, spans[dr][0], spans[0][1]] = halos[(dr, 0)][which]
        for dr in (-1, 0, 1):
            start, stop = spans[dr][0].start, spans[dr][0].stop
            middle = (start + stop) // 2
            for dc in (-1, 1):
                split = to_high if dc < 0 else to_low
                first, second = split(halos[(dr, dc)][which])
                ext[which, start:middle, spans[dc][1]] = first
                ext[which, middle:stop, spans[dc][1]] = second

    row_id = lax.broadcasted_iota(jnp.int32, (SIDE, SIDE), 0)
    col_id = lax.broadcasted_iota(jnp.int32, (SIDE, SIDE), 1)

    def fetch(slot):
        top, left = corner_of(centers, slot, rows, cols)
        row, col = clamped(top, left, rows, cols)
        take = pl.ds(pl.multiple_of((RAD + top - row) // 8 * 8, 8), TALL)
        res, source, target = (buf[slot, take, :] for buf in bufs)
        res, mark = turn_own(res, source, target, lax.rem(RAD + top - row, 8), col - left)
        at_row, at_col = row_id + top, col_id + left
        own = (at_row >= 0) & (at_row < rows) & (at_col >= 0) & (at_col < cols)
        base = pl.multiple_of((left + LANES) // LANES * LANES, LANES)
        back = lax.rem(WIDE + base - left - LANES, WIDE)
        span = pl.ds(pl.multiple_of((top + RAD) // 8 * 8, 8), TALL)
        outer = [
            cut_rows(pltpu.roll(ext[k, span, pl.ds(base, WIDE)], back, 1)[:, :SIDE], lax.rem(top + RAD, 8))
            for k in range(2)
        ]
        signed = jnp.where(own, mark / jnp.where(own, res, 1.0), outer[1])
        return jnp.where(own, res, outer[0]), signed

    def solve_group(group, _):
        def ready(b, _):
            at = group * GROUP + b
            slot = order[jnp.minimum(at, count - 1)]

            @pl.when(at < count)
            def _():
                for copy in copies(slot):
                    copy.wait()

            prepare(b, *fetch(slot))
            return 0

        lax.fori_loop(0, GROUP, ready, 0)
        iterate()

        def done(b, _):
            at = group * GROUP + b

            @pl.when(at < count)
            def _():
                top, left = corner_of(centers, order[at], rows, cols)
                add_window(acc, finish(b), top, left)

            return 0

        lax.fori_loop(0, GROUP, done, 0)
        return 0

    lax.fori_loop(0, (count + GROUP - 1) // GROUP, solve_group, 0)

    def place(slot, _):
        top, left = corner_of(centers, slot, rows, cols)

        @pl.when(is_inner(top, left, rows, cols))
        def _():
            add_window(acc, inner_cur[slot], top, left)

        return 0

    lax.fori_loop(0, live[0], place, 0)
    copy = pltpu.make_async_copy(acc.at[pl.ds(RAD, rows), pl.ds(LANES, cols)], out, out_sem)
    copy.start()
    for dr in (-1, 1):
        outs[(dr, 0)][...] = acc[spans[dr][0], spans[0][1]]
    for dr in (-1, 0, 1):
        for dc in (-1, 1):
            tile = acc[spans[dr][0], spans[dc][1]]
            outs[(dr, dc)][...] = pack_high(tile) if dc < 0 else pack_low(tile)
    copy.wait()


def fold_kernel(rows, cols, *refs):
    halos = dict(zip(SHIFTS, refs[1:9]))
    out, upper, lower, left, right, sems = refs[9:]
    last = cols - LANES
    inner_rows = rows - SIDE
    places = (
        (upper, pl.ds(0, RAD), pl.ds(0, cols)),
        (lower, pl.ds(rows - RAD, RAD), pl.ds(0, cols)),
        (left, pl.ds(RAD, inner_rows), pl.ds(0, LANES)),
        (right, pl.ds(RAD, inner_rows), pl.ds(last, LANES)),
    )
    fetch = [pltpu.make_async_copy(out.at[r, c], buf, sems.at[0, k]) for k, (buf, r, c) in enumerate(places)]
    store = [pltpu.make_async_copy(buf, out.at[r, c], sems.at[1, k]) for k, (buf, r, c) in enumerate(places)]
    for copy in fetch:
        copy.start()

    def spread(dr, dc):
        first, second = (to_low if dc < 0 else to_high)(halos[(dr, dc)][...])
        low = lane_ids(first.shape) < RAD
        keep = low if dc < 0 else jnp.logical_not(low)
        return jnp.where(keep, first, 0.0), jnp.where(keep, second, 0.0)

    for copy in fetch:
        copy.wait()
    half = rows // 2
    for dc, buf, at in ((-1, left, 0), (1, right, last)):
        first, second = spread(0, dc)
        buf[0:half - RAD] = buf[0:half - RAD] + first[RAD:]
        buf[half - RAD:inner_rows] = buf[half - RAD:inner_rows] + second[:half - RAD]
        upper[:, at:at + LANES] = upper[:, at:at + LANES] + first[:RAD]
        lower[:, at:at + LANES] = lower[:, at:at + LANES] + second[half - RAD:]
        for dr, strip in ((-1, upper), (1, lower)):
            one, two = spread(dr, dc)
            strip[:RAD // 2, at:at + LANES] = strip[:RAD // 2, at:at + LANES] + one
            strip[RAD // 2:, at:at + LANES] = strip[RAD // 2:, at:at + LANES] + two
    upper[...] = upper[...] + halos[(-1, 0)][...]
    lower[...] = lower[...] + halos[(1, 0)][...]
    for copy in store:
        copy.start()
    for copy in store:
        copy.wait()


def local(resistance, source_mask, target_mask, centers, live_counts):
    rows, cols = resistance.shape
    slots = centers.shape[0]
    f32, i32 = jnp.float32, jnp.int32
    smem = pl.BlockSpec(memory_space=pltpu.SMEM)
    vmem = pl.BlockSpec(memory_space=pltpu.VMEM)
    hbm = pl.BlockSpec(memory_space=pl.ANY)

    shapes = {
        at: (RAD if at[0] else rows, cols) if at[1] == 0 else ((RAD if at[0] else rows) // 2, LANES) for at in SHIFTS
    }
    pairs = [pltpu.VMEM((2, *shapes[at]), f32) for at in SHIFTS]
    strips = [pltpu.VMEM(shapes[at], f32) for at in SHIFTS]
    state = [pltpu.VMEM((GROUP, SIDE + 16, SIDE), f32)] + [pltpu.VMEM((GROUP, SIDE, SIDE), f32)] * 13
    kinds = (f32, i32, i32)
    frame_shapes = ((rows, LANES), (rows, LANES), (RAD, cols), (RAD, cols))

    windows = pl.pallas_call(
        functools.partial(cut_kernel, rows, cols),
        out_shape=jax.ShapeDtypeStruct((2, slots, SIDE, SIDE), f32),
        in_specs=[smem, smem, hbm, hbm, hbm],
        out_specs=vmem,
        scratch_shapes=[pltpu.VMEM((slots, TALL, WIDE), kind) for kind in kinds]
        + [pltpu.SemaphoreType.DMA((3, slots))],
        compiler_params=pltpu.CompilerParams(vmem_limit_bytes=16 << 20),
        name="cut",
    )(centers, live_counts, resistance, source_mask, target_mask)

    inner_cur, *halos = pl.pallas_call(
        functools.partial(inner_kernel, rows, cols),
        out_shape=[jax.ShapeDtypeStruct((slots, SIDE, SIDE), f32)]
        + [jax.ShapeDtypeStruct((2, *shapes[at]), f32) for at in SHIFTS],
        in_specs=[vmem, hbm, hbm, hbm],
        out_specs=[vmem] * 9,
        scratch_shapes=pairs
        + pairs
        + [pltpu.VMEM(shape, kind) for shape in frame_shapes for kind in kinds]
        + [pltpu.SemaphoreType.DMA((4, 3)), pltpu.SemaphoreType.DMA((8,)), pltpu.SemaphoreType.DMA((8,))]
        + state,
        compiler_params=pltpu.CompilerParams(vmem_limit_bytes=32 << 20, collective_id=0, has_side_effects=True),
        name="inner",
    )(windows, resistance, source_mask, target_mask)

    merged, *currents = pl.pallas_call(
        functools.partial(border_kernel, rows, cols),
        out_shape=[jax.ShapeDtypeStruct((rows, cols), f32)]
        + [jax.ShapeDtypeStruct(shapes[at], f32) for at in SHIFTS],
        in_specs=[smem, smem, vmem, hbm, hbm, hbm] + [vmem] * 8,
        out_specs=[hbm] + [vmem] * 8,
        scratch_shapes=[pltpu.VMEM((slots, TALL + SIDE, WIDE), kind) for kind in kinds]
        + [
            pltpu.SemaphoreType.DMA((3, slots)),
            pltpu.SMEM((slots,), i32),
            pltpu.VMEM((2, rows + SIDE, cols + WIDE), f32),
            pltpu.VMEM((rows + SIDE, cols + WIDE), f32),
            pltpu.SemaphoreType.DMA,
        ]
        + state,
        compiler_params=pltpu.CompilerParams(vmem_limit_bytes=45 << 20),
        name="border",
    )(centers, live_counts, inner_cur, resistance, source_mask, target_mask, *halos)

    back = pl.pallas_call(
        return_kernel,
        out_shape=[jax.ShapeDtypeStruct(shapes[at], f32) for at in SHIFTS],
        in_specs=[vmem] * 8,
        out_specs=[vmem] * 8,
        scratch_shapes=strips + [pltpu.SemaphoreType.DMA((8,)), pltpu.SemaphoreType.DMA((8,))],
        compiler_params=pltpu.CompilerParams(vmem_limit_bytes=8 << 20, collective_id=1, has_side_effects=True),
        name="give_back",
    )(*currents)
    out_shape = jax.ShapeDtypeStruct((rows, cols), f32)

    return pl.pallas_call(
        functools.partial(fold_kernel, rows, cols),
        out_shape=out_shape,
        in_specs=[hbm] + [vmem] * 8,
        out_specs=hbm,
        scratch_shapes=[
            pltpu.VMEM((RAD, cols), f32),
            pltpu.VMEM((RAD, cols), f32),
            pltpu.VMEM((rows - SIDE, LANES), f32),
            pltpu.VMEM((rows - SIDE, LANES), f32),
            pltpu.SemaphoreType.DMA((2, 4)),
        ],
        input_output_aliases={0: 0},
        compiler_params=pltpu.CompilerParams(vmem_limit_bytes=16 << 20),
        name="fold",
    )(merged, *back)


def solution(mesh):
    return jax.shard_map(
        local,
        mesh=mesh,
        in_specs=(
            P("row", "col"),
            P("row", "col"),
            P("row", "col"),
            P(("row", "col"), None),
            P(("row", "col")),
        ),
        out_specs=P("row", "col"),
        check_vma=False,
    )
```

```python
import functools

import jax
import jax.numpy as jnp
from jax import lax
from jax.experimental import pallas as pl
from jax.experimental.pallas import tpu as pltpu
from jax.sharding import PartitionSpec as P

RAD = 64
SIDE = 2 * RAD
ITERS = 24
LEAKAGE = 0.02
INNER_GROUP = 8
BORDER_GROUP = 4
CHUNK = 32
LANES = 128
TALL = SIDE + 8
WIDE = 2 * LANES
SHIFTS = ((0, -1), (0, 1), (-1, 0), (1, 0), (-1, -1), (-1, 1), (1, -1), (1, 1))


def roll(value, shift, axis):
    return pltpu.roll(value, shift % value.shape[axis], axis)


def lane_ids(shape):
    return lax.broadcasted_iota(jnp.int32, shape, 1)


def to_low(packed):
    return packed, roll(packed, RAD, 1)


def to_high(packed):
    return roll(packed, RAD, 1), packed


def pack_low(tile):
    half = tile.shape[0] // 2
    first, second = tile[:half], tile[half:]
    return jnp.where(lane_ids(first.shape) < RAD, first, roll(second, RAD, 1))


def pack_high(tile):
    half = tile.shape[0] // 2
    first, second = tile[:half], tile[half:]
    return jnp.where(lane_ids(first.shape) < RAD, roll(first, RAD, 1), second)


def neighbours():
    row, col = lax.axis_index("row"), lax.axis_index("col")
    rows, cols = lax.axis_size("row"), lax.axis_size("col")
    found = {}
    for (dr, dc) in SHIFTS:
        r, c = row + dr, col + dc
        found[(dr, dc)] = ((r >= 0) & (r < rows) & (c >= 0) & (c < cols), (r, c))
    return found


def greet(found):
    barrier = pltpu.get_barrier_semaphore()
    for at in SHIFTS:
        exists, device = found[at]

        @pl.when(exists)
        def _():
            pl.semaphore_signal(barrier, inc=1, device_id=device, device_id_type=pl.DeviceIdType.MESH)


def all_greeted(found):
    count = sum(found[at][0].astype(jnp.int32) for at in SHIFTS)
    pl.semaphore_wait(pltpu.get_barrier_semaphore(), count)


def transfers(found, pieces, halos, send_sems, recv_sems):
    made = []
    for k, at in enumerate(SHIFTS):
        exists, device = found[at]
        back = (-at[0], -at[1])
        made.append((exists, pltpu.make_async_remote_copy(
            src_ref=pieces[at],
            dst_ref=halos[back],
            send_sem=send_sems.at[k],
            recv_sem=recv_sems.at[SHIFTS.index(back)],
            device_id=device,
            device_id_type=pl.DeviceIdType.MESH,
        )))
    return made


def landings(found, pieces, halos, send_sems, recv_sems):
    made = []
    for k, at in enumerate(SHIFTS):
        exists, device = found[at]
        made.append((exists, pltpu.make_async_remote_copy(
            src_ref=pieces[at],
            dst_ref=halos[at],
            send_sem=send_sems.at[k],
            recv_sem=recv_sems.at[k],
            device_id=device,
            device_id_type=pl.DeviceIdType.MESH,
        )))
    return made


def start_all(copies):
    for exists, copy in copies:
        pl.when(exists)(copy.start)


def finish_all(copies, arrivals):
    for exists, copy in copies:
        pl.when(exists)(copy.wait_send)
    for exists, copy in arrivals:
        pl.when(exists)(copy.wait_recv)


def corner_of(centers, slot, rows, cols):
    return lax.rem(centers[slot, 0], rows) - RAD, lax.rem(centers[slot, 1], cols) - RAD


def is_inner(top, left, rows, cols):
    return (top >= 0) & (top <= rows - SIDE) & (left >= 0) & (left <= cols - SIDE)


def clamped(top, left, rows, cols):
    row = jnp.clip((top + RAD) // 8 * 8 - RAD, 0, rows - TALL)
    col = jnp.clip((left + LANES) // LANES * LANES - LANES, 0, cols - WIDE)
    return pl.multiple_of(row, 8), pl.multiple_of(col, LANES)


def total(values):
    return jnp.sum(jnp.sum(values, axis=0, keepdims=True), axis=1, keepdims=True)


def cut_rows(value, skip):
    return pltpu.roll(value, lax.rem(TALL - skip, TALL), 0)[:SIDE]


def add_window(acc, current, top, left):
    col = pl.multiple_of((left + LANES) // LANES * LANES, LANES)
    shift = left + LANES - col
    wide = jnp.concatenate([current, jnp.zeros_like(current)], axis=1)
    wide = pltpu.roll(wide, shift, 1)
    wide = jnp.concatenate([wide, jnp.zeros((8, WIDE), jnp.float32)], axis=0)
    wide = pltpu.roll(wide, lax.rem(top + RAD, 8), 0)
    rows = pl.ds(pl.multiple_of((top + RAD) // 8 * 8, 8), TALL)
    acc[rows, pl.ds(col, WIDE)] = acc[rows, pl.ds(col, WIDE)] + wide


def solver_parts(state, group_size):
    r_s, p_s, s_s, x_s, w_s, vd_s, vu_s, hr_s, hl_s, isd_s, inj_s, gnd_s, v_s, h_s = state
    row_id = lax.broadcasted_iota(jnp.int32, (SIDE, SIDE), 0)
    col_id = lax.broadcasted_iota(jnp.int32, (SIDE, SIDE), 1)

    def operate(b):
        squares = jnp.zeros((8, SIDE), jnp.float32)
        products = jnp.zeros((8, SIDE), jnp.float32)
        for at in range(0, SIDE, CHUNK):
            cut = slice(at, at + CHUNK)
            here = r_s[b, at + 8:at + 8 + CHUNK, :]
            beside = vd_s[b, cut] * r_s[b, at + 9:at + 9 + CHUNK, :] + vu_s[b, cut] * r_s[b, at + 7:at + 7 + CHUNK, :]
            beside = beside + hr_s[b, cut] * roll(here, -1, 1) + hl_s[b, cut] * roll(here, 1, 1)
            applied = here - beside
            w_s[b, cut] = applied
            squares = squares + jnp.sum((here * here).reshape(CHUNK // 8, 8, SIDE), axis=0)
            products = products + jnp.sum((here * applied).reshape(CHUNK // 8, 8, SIDE), axis=0)
        return total(squares), total(products)

    def prepare(b, res, signed):
        res_down, res_right = roll(res, -1, 0), roll(res, -1, 1)
        has_down = (res > 0.0) & (res_down > 0.0) & (row_id < SIDE - 1)
        has_right = (res > 0.0) & (res_right > 0.0) & (col_id < SIDE - 1)
        vertical = jnp.where(has_down, 2.0 / jnp.where(has_down, res + res_down, 1.0), 0.0)
        horizontal = jnp.where(has_right, 2.0 / jnp.where(has_right, res + res_right, 1.0), 0.0)
        center = ((row_id == RAD) & (col_id == RAD)).astype(jnp.float32)
        inject = jnp.maximum(signed, 0.0) + center
        ground = jnp.maximum(-signed, 0.0)
        diagonal = vertical + roll(vertical, 1, 0) + horizontal + roll(horizontal, 1, 1) + ground + LEAKAGE
        isd = 1.0 / jnp.sqrt(diagonal)
        scaled_v = vertical * isd * roll(isd, -1, 0)
        scaled_h = horizontal * isd * roll(isd, -1, 1)
        v_s[b], h_s[b] = vertical, horizontal
        vd_s[b], vu_s[b] = scaled_v, roll(scaled_v, 1, 0)
        hr_s[b], hl_s[b] = scaled_h, roll(scaled_h, 1, 1)
        inj_s[b], gnd_s[b], isd_s[b] = inject, ground, isd
        r_s[b, 0:8, :] = jnp.zeros((8, SIDE), jnp.float32)
        r_s[b, 8 + SIDE:16 + SIDE, :] = jnp.zeros((8, SIDE), jnp.float32)
        r_s[b, 8:8 + SIDE, :] = inject * isd
        zero = jnp.zeros((SIDE, SIDE), jnp.float32)
        p_s[b], s_s[b], x_s[b] = zero, zero, zero

    def step(_, carry):
        after = []
        for b in range(group_size):
            alpha, beta, gamma_inv, alpha_inv = carry[b]
            for at in range(0, SIDE, CHUNK):
                cut, inset = slice(at, at + CHUNK), slice(at + 8, at + 8 + CHUNK)
                here = r_s[b, inset]
                direction = here + beta * p_s[b, cut]
                applied = w_s[b, cut] + beta * s_s[b, cut]
                p_s[b, cut] = direction
                s_s[b, cut] = applied
                x_s[b, cut] = x_s[b, cut] + alpha * direction
                r_s[b, inset] = here - alpha * applied
            gamma, delta = operate(b)
            beta = gamma * gamma_inv
            bottom = delta - beta * (gamma * alpha_inv)
            gamma_inv = 1.0 / gamma
            after.append((gamma / bottom, beta, gamma_inv, bottom * gamma_inv))
        return tuple(after)

    def finish(b):
        isd, vertical, horizontal = isd_s[b], v_s[b], h_s[b]
        voltage = x_s[b] * isd
        flow_down = vertical * jnp.abs(voltage - roll(voltage, -1, 0))
        flow_right = horizontal * jnp.abs(voltage - roll(voltage, -1, 1))
        flow = flow_down + roll(flow_down, 1, 0) + flow_right + roll(flow_right, 1, 1)
        return 0.5 * (flow + inj_s[b] + gnd_s[b] * jnp.abs(voltage))

    def iterate():
        carry = []
        for b in range(group_size):
            gamma, delta = operate(b)
            gamma_inv = 1.0 / gamma
            carry.append((gamma / delta, jnp.zeros_like(gamma), gamma_inv, delta * gamma_inv))
        lax.fori_loop(0, ITERS, step, tuple(carry), unroll=2)

    return prepare, iterate, finish


def spans_of(rows, cols):
    return {
        -1: (slice(0, RAD), slice(0, LANES)),
        0: (slice(RAD, RAD + rows), slice(LANES, LANES + cols)),
        1: (slice(RAD + rows, SIDE + rows), slice(LANES + cols, WIDE + cols)),
    }


def turn_own(res, source, target, skip, turn):
    source, target = source.astype(jnp.float32), target.astype(jnp.float32)
    mark = source - target * (1.0 - source)
    turn = lax.rem(WIDE + turn, WIDE)
    res = cut_rows(pltpu.roll(res, turn, 1)[:, :SIDE], skip)
    mark = cut_rows(pltpu.roll(mark, turn, 1)[:, :SIDE], skip)
    return res, mark


def cut_kernel(rows, cols, centers, live, *refs):
    raw, out, bufs, sems = refs[:3], refs[3], refs[4:7], refs[7]

    def place(slot):
        top, left = corner_of(centers, slot, rows, cols)
        return top, left, *clamped(top, left, rows, cols)

    def copies(slot):
        _, _, row, col = place(slot)
        return [
            pltpu.make_async_copy(src.at[pl.ds(row, TALL), pl.ds(col, WIDE)], dst.at[slot], sems.at[k, slot])
            for k, (src, dst) in enumerate(zip(raw, bufs))
        ]

    def begin(slot, _):
        for copy in copies(slot):
            copy.start()
        return 0

    def cut(slot, _):
        for copy in copies(slot):
            copy.wait()
        top, left, row, col = place(slot)
        res, mark = turn_own(*(buf[slot] for buf in bufs), top - row, col - left)
        out[0, slot] = res
        out[1, slot] = mark / res
        return 0

    lax.fori_loop(0, live[0], begin, 0)
    lax.fori_loop(0, live[0], cut, 0)


def inner_kernel(rows, cols, windows, *refs):
    raw = refs[:3]
    cur, outs = refs[3], dict(zip(SHIFTS, refs[4:12]))
    pieces, halos = dict(zip(SHIFTS, refs[12:20])), dict(zip(SHIFTS, refs[20:28]))
    frames = [refs[28 + 3 * k:31 + 3 * k] for k in range(4)]
    sems, send_sems, recv_sems = refs[40:43]
    prepare, iterate, finish = solver_parts(refs[43:], INNER_GROUP)
    slots = windows.shape[1]
    found = neighbours()

    everything = pl.ds(0, rows)
    places = (
        (everything, pl.ds(0, LANES)),
        (everything, pl.ds(cols - LANES, LANES)),
        (pl.ds(0, RAD), pl.ds(0, cols)),
        (pl.ds(rows - RAD, RAD), pl.ds(0, cols)),
    )
    frame_copies = [
        [pltpu.make_async_copy(raw[k].at[places[f]], frames[f][k], sems.at[f, k]) for k in range(3)]
        for f in range(4)
    ]
    for copy in sum(frame_copies, []):
        copy.start()
    for at in SHIFTS:
        halos[at][...] = jnp.zeros_like(halos[at])
    greet(found)

    def strengths(frame, cut=slice(None)):
        res, source, target = (ref[cut] for ref in frame)
        source, target = source.astype(jnp.float32), target.astype(jnp.float32)
        conduct = 1.0 / res
        return res, source * conduct - target * (1.0 - source) * conduct

    for f, at in enumerate(((0, -1), (0, 1), (-1, 0), (1, 0))):
        for copy in frame_copies[f]:
            copy.wait()
        for k, value in enumerate(strengths(frames[f])):
            if at[1] == 0:
                pieces[at][k] = value
            else:
                squeeze = pack_low if at[1] < 0 else pack_high
                pieces[at][k] = squeeze(value)
                pieces[(-1, at[1])][k] = squeeze(value[:RAD])
                pieces[(1, at[1])][k] = squeeze(value[rows - RAD:])
    all_greeted(found)
    copies = transfers(found, pieces, halos, send_sems, recv_sems)
    start_all(copies)

    def solve_group(group, _):
        def ready(b, _):
            slot = group * INNER_GROUP + b
            prepare(b, windows[0, slot], windows[1, slot])
            return 0

        lax.fori_loop(0, INNER_GROUP, ready, 0)
        iterate()

        def done(b, _):
            cur[group * INNER_GROUP + b] = finish(b)
            return 0

        lax.fori_loop(0, INNER_GROUP, done, 0)
        return 0

    lax.fori_loop(0, slots // INNER_GROUP, solve_group, 0)
    finish_all(copies, landings(found, pieces, halos, send_sems, recv_sems))
    for at in SHIFTS:
        outs[at][...] = halos[at][...]


def return_kernel(*refs):
    pieces, outs, halos = (dict(zip(SHIFTS, refs[8 * k:8 * k + 8])) for k in range(3))
    send_sems, recv_sems = refs[24:]
    found = neighbours()
    for at in SHIFTS:
        halos[at][...] = jnp.zeros_like(halos[at])
    greet(found)
    all_greeted(found)
    copies = transfers(found, pieces, halos, send_sems, recv_sems)
    start_all(copies)
    finish_all(copies, landings(found, pieces, halos, send_sems, recv_sems))
    for at in SHIFTS:
        outs[at][...] = halos[at][...]


def border_kernel(rows, cols, centers, live, inner_cur, *refs):
    raw, halos = refs[:3], dict(zip(SHIFTS, refs[3:11]))
    out, outs = refs[11], dict(zip(SHIFTS, refs[12:20]))
    bufs, sems, order, ext, acc, out_sem = refs[20:23], *refs[23:28]
    prepare, iterate, finish = solver_parts(refs[28:], BORDER_GROUP)

    def copies(slot):
        top, left = corner_of(centers, slot, rows, cols)
        row, col = clamped(top, left, rows, cols)
        return [
            pltpu.make_async_copy(
                src.at[pl.ds(row, TALL), pl.ds(col, WIDE)],
                dst.at[slot, pl.ds(RAD, TALL), :],
                sems.at[k, slot],
            )
            for k, (src, dst) in enumerate(zip(raw, bufs))
        ]

    def classify(slot, count):
        top, left = corner_of(centers, slot, rows, cols)
        outer = jnp.logical_not(is_inner(top, left, rows, cols))

        @pl.when(outer)
        def _():
            order[count] = slot
            for copy in copies(slot):
                copy.start()

        return count + outer.astype(jnp.int32)

    count = lax.fori_loop(0, live[0], classify, jnp.int32(0))
    acc[...] = jnp.zeros_like(acc)
    spans = spans_of(rows, cols)
    for which in range(2):
        for dr in (-1, 1):
            ext[which, spans[dr][0], spans[0][1]] = halos[(dr, 0)][which]
        for dr in (-1, 0, 1):
            start, stop = spans[dr][0].start, spans[dr][0].stop
            middle = (start + stop) // 2
            for dc in (-1, 1):
                split = to_high if dc < 0 else to_low
                first, second = split(halos[(dr, dc)][which])
                ext[which, start:middle, spans[dc][1]] = first
                ext[which, middle:stop, spans[dc][1]] = second

    row_id = lax.broadcasted_iota(jnp.int32, (SIDE, SIDE), 0)
    col_id = lax.broadcasted_iota(jnp.int32, (SIDE, SIDE), 1)

    def fetch(slot):
        top, left = corner_of(centers, slot, rows, cols)
        row, col = clamped(top, left, rows, cols)
        take = pl.ds(pl.multiple_of((RAD + top - row) // 8 * 8, 8), TALL)
        res, source, target = (buf[slot, take, :] for buf in bufs)
        res, mark = turn_own(res, source, target, lax.rem(RAD + top - row, 8), col - left)
        at_row, at_col = row_id + top, col_id + left
        own = (at_row >= 0) & (at_row < rows) & (at_col >= 0) & (at_col < cols)
        base = pl.multiple_of((left + LANES) // LANES * LANES, LANES)
        back = lax.rem(WIDE + base - left - LANES, WIDE)
        span = pl.ds(pl.multiple_of((top + RAD) // 8 * 8, 8), TALL)
        outer = [
            cut_rows(pltpu.roll(ext[k, span, pl.ds(base, WIDE)], back, 1)[:, :SIDE], lax.rem(top + RAD, 8))
            for k in range(2)
        ]
        signed = jnp.where(own, mark / jnp.where(own, res, 1.0), outer[1])
        return jnp.where(own, res, outer[0]), signed

    def solve_group(group, _):
        def ready(b, _):
            at = group * BORDER_GROUP + b
            slot = order[jnp.minimum(at, count - 1)]

            @pl.when(at < count)
            def _():
                for copy in copies(slot):
                    copy.wait()

            prepare(b, *fetch(slot))
            return 0

        lax.fori_loop(0, BORDER_GROUP, ready, 0)
        iterate()

        def done(b, _):
            at = group * BORDER_GROUP + b

            @pl.when(at < count)
            def _():
                top, left = corner_of(centers, order[at], rows, cols)
                add_window(acc, finish(b), top, left)

            return 0

        lax.fori_loop(0, BORDER_GROUP, done, 0)
        return 0

    lax.fori_loop(0, (count + BORDER_GROUP - 1) // BORDER_GROUP, solve_group, 0)

    def place(slot, _):
        top, left = corner_of(centers, slot, rows, cols)

        @pl.when(is_inner(top, left, rows, cols))
        def _():
            add_window(acc, inner_cur[slot], top, left)

        return 0

    lax.fori_loop(0, live[0], place, 0)
    copy = pltpu.make_async_copy(acc.at[pl.ds(RAD, rows), pl.ds(LANES, cols)], out, out_sem)
    copy.start()
    for dr in (-1, 1):
        outs[(dr, 0)][...] = acc[spans[dr][0], spans[0][1]]
    for dr in (-1, 0, 1):
        for dc in (-1, 1):
            tile = acc[spans[dr][0], spans[dc][1]]
            outs[(dr, dc)][...] = pack_high(tile) if dc < 0 else pack_low(tile)
    copy.wait()


def fold_kernel(rows, cols, *refs):
    halos = dict(zip(SHIFTS, refs[1:9]))
    out, upper, lower, left, right, sems = refs[9:]
    last = cols - LANES
    inner_rows = rows - SIDE
    places = (
        (upper, pl.ds(0, RAD), pl.ds(0, cols)),
        (lower, pl.ds(rows - RAD, RAD), pl.ds(0, cols)),
        (left, pl.ds(RAD, inner_rows), pl.ds(0, LANES)),
        (right, pl.ds(RAD, inner_rows), pl.ds(last, LANES)),
    )
    fetch = [pltpu.make_async_copy(out.at[r, c], buf, sems.at[0, k]) for k, (buf, r, c) in enumerate(places)]
    store = [pltpu.make_async_copy(buf, out.at[r, c], sems.at[1, k]) for k, (buf, r, c) in enumerate(places)]
    for copy in fetch:
        copy.start()

    def spread(dr, dc):
        first, second = (to_low if dc < 0 else to_high)(halos[(dr, dc)][...])
        low = lane_ids(first.shape) < RAD
        keep = low if dc < 0 else jnp.logical_not(low)
        return jnp.where(keep, first, 0.0), jnp.where(keep, second, 0.0)

    for copy in fetch:
        copy.wait()
    half = rows // 2
    for dc, buf, at in ((-1, left, 0), (1, right, last)):
        first, second = spread(0, dc)
        buf[0:half - RAD] = buf[0:half - RAD] + first[RAD:]
        buf[half - RAD:inner_rows] = buf[half - RAD:inner_rows] + second[:half - RAD]
        upper[:, at:at + LANES] = upper[:, at:at + LANES] + first[:RAD]
        lower[:, at:at + LANES] = lower[:, at:at + LANES] + second[half - RAD:]
        for dr, strip in ((-1, upper), (1, lower)):
            one, two = spread(dr, dc)
            strip[:RAD // 2, at:at + LANES] = strip[:RAD // 2, at:at + LANES] + one
            strip[RAD // 2:, at:at + LANES] = strip[RAD // 2:, at:at + LANES] + two
    upper[...] = upper[...] + halos[(-1, 0)][...]
    lower[...] = lower[...] + halos[(1, 0)][...]
    for copy in store:
        copy.start()
    for copy in store:
        copy.wait()


def local(resistance, source_mask, target_mask, centers, live_counts):
    rows, cols = resistance.shape
    slots = centers.shape[0]
    f32, i32 = jnp.float32, jnp.int32
    smem = pl.BlockSpec(memory_space=pltpu.SMEM)
    vmem = pl.BlockSpec(memory_space=pltpu.VMEM)
    hbm = pl.BlockSpec(memory_space=pltpu.HBM)

    shapes = {
        at: (RAD if at[0] else rows, cols) if at[1] == 0 else ((RAD if at[0] else rows) // 2, LANES) for at in SHIFTS
    }
    pairs = [pltpu.VMEM((2, *shapes[at]), f32) for at in SHIFTS]
    strips = [pltpu.VMEM(shapes[at], f32) for at in SHIFTS]

    def state(group_size):
        return [pltpu.VMEM((group_size, SIDE + 16, SIDE), f32)] + [pltpu.VMEM((group_size, SIDE, SIDE), f32)] * 13

    kinds = (f32, i32, i32)
    frame_shapes = ((rows, LANES), (rows, LANES), (RAD, cols), (RAD, cols))

    windows = pl.pallas_call(
        functools.partial(cut_kernel, rows, cols),
        out_shape=jax.ShapeDtypeStruct((2, slots, SIDE, SIDE), f32),
        in_specs=[smem, smem, hbm, hbm, hbm],
        out_specs=vmem,
        scratch_shapes=[pltpu.VMEM((slots, TALL, WIDE), kind) for kind in kinds]
        + [pltpu.SemaphoreType.DMA((3, slots))],
        compiler_params=pltpu.CompilerParams(vmem_limit_bytes=60 << 20),
        name="cut",
    )(centers, live_counts, resistance, source_mask, target_mask)

    inner_cur, *halos = pl.pallas_call(
        functools.partial(inner_kernel, rows, cols),
        out_shape=[jax.ShapeDtypeStruct((slots, SIDE, SIDE), f32)]
        + [jax.ShapeDtypeStruct((2, *shapes[at]), f32) for at in SHIFTS],
        in_specs=[vmem, hbm, hbm, hbm],
        out_specs=[vmem] * 9,
        scratch_shapes=pairs
        + pairs
        + [pltpu.VMEM(shape, kind) for shape in frame_shapes for kind in kinds]
        + [pltpu.SemaphoreType.DMA((4, 3)), pltpu.SemaphoreType.DMA((8,)), pltpu.SemaphoreType.DMA((8,))]
        + state(INNER_GROUP),
        compiler_params=pltpu.CompilerParams(vmem_limit_bytes=60 << 20, collective_id=0, has_side_effects=True),
        name="inner",
    )(windows, resistance, source_mask, target_mask)

    merged, *currents = pl.pallas_call(
        functools.partial(border_kernel, rows, cols),
        out_shape=[jax.ShapeDtypeStruct((rows, cols), f32)]
        + [jax.ShapeDtypeStruct(shapes[at], f32) for at in SHIFTS],
        in_specs=[smem, smem, vmem, hbm, hbm, hbm] + [vmem] * 8,
        out_specs=[hbm] + [vmem] * 8,
        scratch_shapes=[pltpu.VMEM((slots, TALL + SIDE, WIDE), kind) for kind in kinds]
        + [
            pltpu.SemaphoreType.DMA((3, slots)),
            pltpu.SMEM((slots,), i32),
            pltpu.VMEM((2, rows + SIDE, cols + WIDE), f32),
            pltpu.VMEM((rows + SIDE, cols + WIDE), f32),
            pltpu.SemaphoreType.DMA,
        ]
        + state(BORDER_GROUP),
        compiler_params=pltpu.CompilerParams(vmem_limit_bytes=45 << 20),
        name="border",
    )(centers, live_counts, inner_cur, resistance, source_mask, target_mask, *halos)

    back = pl.pallas_call(
        return_kernel,
        out_shape=[jax.ShapeDtypeStruct(shapes[at], f32) for at in SHIFTS],
        in_specs=[vmem] * 8,
        out_specs=[vmem] * 8,
        scratch_shapes=strips + [pltpu.SemaphoreType.DMA((8,)), pltpu.SemaphoreType.DMA((8,))],
        compiler_params=pltpu.CompilerParams(vmem_limit_bytes=8 << 20, collective_id=1, has_side_effects=True),
        name="give_back",
    )(*currents)
    out_shape = jax.ShapeDtypeStruct((rows, cols), f32)

    return pl.pallas_call(
        functools.partial(fold_kernel, rows, cols),
        out_shape=out_shape,
        in_specs=[hbm] + [vmem] * 8,
        out_specs=hbm,
        scratch_shapes=[
            pltpu.VMEM((RAD, cols), f32),
            pltpu.VMEM((RAD, cols), f32),
            pltpu.VMEM((rows - SIDE, LANES), f32),
            pltpu.VMEM((rows - SIDE, LANES), f32),
            pltpu.SemaphoreType.DMA((2, 4)),
        ],
        input_output_aliases={0: 0},
        compiler_params=pltpu.CompilerParams(vmem_limit_bytes=16 << 20),
        name="fold",
    )(merged, *back)


def solution(mesh):
    return jax.shard_map(
        local,
        mesh=mesh,
        in_specs=(
            P("row", "col"),
            P("row", "col"),
            P("row", "col"),
            P(("row", "col"), None),
            P(("row", "col")),
        ),
        out_specs=P("row", "col"),
        check_vma=False,
    )
```
